32 devices in a mesh: group: 4 (over x, core), seq: 2 (over y), expert: 4 (over z).
Axes of the slice: x: 2, y: 2, z: 4, core: 2. Of those that a mesh axis runs over, the one named last changes fastest.
Arguments:
- queries: bfloat16 [16, 32, 128], P('expert', 'group')
- keys: bfloat16 [16, 256, 8, 128], P('expert', 'seq', 'group')
- values: bfloat16 [16, 256, 8, 128], P('expert', 'seq', 'group'), may hold values from -48 to 48
- block_of_slot: int32 [16, 16], P('expert', 'seq'), may hold values from 0 to 15, each once within a row
- lengths: int32 [16], P('expert'), may hold values from 128 to 256
- out_proj: bfloat16 [4096, 4096], P('group', 'seq'), may hold values from -0.09375 to 0.09375
- residual: bfloat16 [16, 4096], P('expert', 'seq'), may hold values from -6 to 6
- norm_gain: bfloat16 [4096], replicated, may hold values from 0.25 to 1.75
- router: bfloat16 [4096, 8], replicated, may hold values from -0.09375 to 0.09375
- routes: int32 [16, 2], P('expert'), may hold values from 0 to 7, all different within a row; in each aligned block of 4 rows (0 to 3, 4 to 7, ...) at most 2 rows name the same one
- w_gate: bfloat16 [8, 4096, 14336], P('expert', None, ('group', 'seq')), may hold values from -0.09375 to 0.09375
- w_up: bfloat16 [8, 4096, 14336], P('expert', None, ('group', 'seq')), may hold values from -0.09375 to 0.09375
- w_down: bfloat16 [8, 14336, 4096], P('expert', ('group', 'seq')), may hold values from -0.046875 to 0.046875
Outputs:
- layer_out: bfloat16 [16, 4096], P('expert', 'seq')
The draws below stay inside these ranges and needn't reach their ends.
Inputs may be any that keep to these rules, and one draw needn't show every extreme that they name: `block_of_slot`: each row lists every logical block once. `routes`: the two ids of a row differ; among the 4 rows of one device no expert is named more than 2 times, and in some such blocks one expert is named exactly 2 times.
All inputs are finite; a program needn't handle non-finite values.
Results may differ from the reference program's by a relative error of at most 0.013.
Values may be sent and summed in bfloat16 or wider, within the bound.
No kernel may reach another device: no remote copies, remote signals or barrier semaphores. Data moves between devices by JAX's collectives and lax.ppermute only.
A program may use at most 128 MiB of HBM per device.

```python
import math
import jax
import jax.numpy as jnp
import numpy as np
from jax import lax

D = 4096
FF = 14336
HEADS = 32
KV_HEADS = 8
HEAD_DIM = 128
EXPERTS = 8
TOPK = 2
BLOCK = 16
REQ_DEV = 4
CAPACITY = 2
REQUESTS = 16
CONTEXT = 256
SLOTS = 16


def shared_keys(key):
    return jax.random.normal(jax.random.fold_in(key, 11), (REQUESTS, CONTEXT, KV_HEADS, HEAD_DIM), jnp.float32)


def draw_keys(key, part):
    base = shared_keys(key)
    return base.astype(jnp.bfloat16)


def draw_queries(key, part):
    base = jax.random.normal(jax.random.fold_in(key, 22), (REQUESTS, HEADS, HEAD_DIM), jnp.float32)
    return base.astype(jnp.bfloat16)


def touch_ends(array, stream_key, smallest, high):
    spot = [jax.random.randint(jax.random.fold_in(stream_key, axis), (), 0, length) for axis, length in enumerate(array.shape)]
    longest = array.shape.index(max(array.shape))
    neighbour = spot[:longest] + [(spot[longest] + 1) % array.shape[longest]] + spot[longest + 1:]
    return array.at[tuple(spot)].set(smallest).at[tuple(neighbour)].set(high)


def levels(own_key, dims, shards, smallest, largest):
    def one(dim, parts):
        steps = jax.random.uniform(jax.random.fold_in(jax.random.fold_in(own_key, 6), dim), (parts,), jnp.float32, smallest / len(shards), largest / len(shards))
        return jnp.repeat(jnp.exp(steps), dims[dim] // parts).reshape((-1,) + (1,) * (len(dims) - dim - 1))

    level = one(*shards[0])
    for cut in shards[1:]:
        level = level * one(*cut)
    return level


def routed_block(own_key, own, number, rows, count, top, bound, skew):
    ranking = jax.random.permutation(own_key, count)
    heavy_load, common = shares(count, rows * top, bound, skew, True), shares(count, rows * top, bound, skew, False)
    places = jnp.arange(count)

    def named(sizes, rotation):
        used = int((sizes > 0).sum())
        fixed = max(1, used // 4)
        passed = fixed + (places - fixed + rotation * (used - fixed)) % max(1, count - fixed)
        return jnp.zeros((count,), jnp.int32).at[ranking[jnp.where(places < fixed, places, passed)]].set(jnp.asarray(sizes, jnp.int32))

    sizes = jnp.where(number % 4 == 0, named(heavy_load, number // 4), named(common, number - number // 4 - 1))
    mixed = jax.random.permutation(jax.random.fold_in(own, 3), count)
    source_of, receiver = mixed[0:count // 2 * 2:2], mixed[1:count // 2 * 2:2]
    slack = jnp.minimum(sizes[source_of] - 1, bound - sizes[receiver]) // 2
    slack = jnp.where((source_of == ranking[0]) | (receiver == ranking[0]) | (sizes[receiver] == 0), 0, jnp.maximum(slack, 0))
    passed = jax.random.randint(jax.random.fold_in(own, 4), (count // 2,), 0, 1 << 20) % (slack + 1)
    sizes = sizes.at[source_of].add(-passed).at[receiver].add(passed)
    labels = jnp.searchsorted(jnp.cumsum(sizes), jnp.arange(rows * top), side="right").astype(jnp.int32)
    listing = labels.reshape(top, rows).T
    listing = listing[jax.random.permutation(jax.random.fold_in(own, 1), rows)]
    rotation = jax.random.randint(jax.random.fold_in(own, 2), (rows, 1), 0, top)
    return jnp.take_along_axis(listing, (jnp.arange(top)[None, :] + rotation) % top, axis=1)


def shares(amount, total, limit, lean, full):
    weights = [(1 << 20) // math.isqrt(rank ** lean) + 1 for rank in range(1, amount + 1)]
    largest = limit if full else min(limit, max(-(-total // amount), total * weights[0] // sum(weights)))
    least = 1 if total - largest >= amount - 1 else 0
    given, rest = [largest] + [least] * (amount - 1), total - largest - least * (amount - 1)
    while rest > 0:
        candidates = [i for i in range(1, amount) if given[i] < largest] or [i for i in range(1, amount) if given[i] < limit]
        pool, remaining = sum([weights[i] for i in candidates]), rest
        for i in candidates:
            extra = min(limit - given[i], max(1, remaining * weights[i] // pool), rest)
            given[i] = given[i] + extra
            rest = rest - extra
    return np.array(given)


def noise(stream_key, extent, scale, limit, split=(), kind=jnp.bfloat16):
    array = scale * jax.random.normal(stream_key, extent, jnp.float32)
    if split:
        array = array * levels(stream_key, extent, split, -0.22, 0.18)
    return jnp.clip(array, -limit, limit).astype(kind)


def setup_inputs(seed: int = 0) -> dict:
    arg_keys = jax.random.split(jax.random.key(seed), 14)
    queries = draw_queries(jax.random.fold_in(arg_keys[13], 71), 0)
    keys = draw_keys(jax.random.fold_in(arg_keys[13], 71), 0)
    values = noise(arg_keys[2], (REQUESTS, CONTEXT, KV_HEADS, HEAD_DIM), 8.0, 48.0, ((0, 4), (1, 2), (2, 4)))
    block_of_slot = jax.vmap(lambda own: jax.random.permutation(own, SLOTS))(jax.random.split(arg_keys[3], REQUESTS)).reshape((REQUESTS, SLOTS)).astype(jnp.int32)
    lengths = touch_ends(jax.random.randint(arg_keys[4], (REQUESTS,), CONTEXT // 2, CONTEXT + 1), jax.random.fold_in(arg_keys[4], 1), CONTEXT // 2, CONTEXT).astype(jnp.int32)
    out_proj = noise(arg_keys[5], (HEADS * HEAD_DIM, D), (HEADS * HEAD_DIM) ** -0.5, 0.09375, ((0, 4), (1, 2)))
    residual = noise(arg_keys[6], (REQUESTS, D), 1.0, 6.0, ((0, 4), (1, 2)))
    norm_gain = jnp.clip(1.0 + 0.15 * jax.random.normal(arg_keys[7], (D,), jnp.float32), 0.25, 1.75).astype(jnp.bfloat16)
    router = noise(arg_keys[8], (D, EXPERTS), D ** -0.5, 0.09375)
    routes_keys = jax.random.split(jax.random.fold_in(arg_keys[9], 1), REQUESTS // REQ_DEV)
    routes_turns = jax.random.permutation(jax.random.fold_in(arg_keys[9], 3), REQUESTS // REQ_DEV)
    routes = jax.vmap(lambda own, number: routed_block(jax.random.fold_in(arg_keys[9], 2), own, number, REQ_DEV, EXPERTS, TOPK, CAPACITY, 1))(routes_keys, routes_turns).reshape((REQUESTS, TOPK))
    w_gate = noise(arg_keys[10], (EXPERTS, D, FF), D ** -0.5, 0.09375, ((0, 4), (2, 8)))
    w_up = noise(arg_keys[11], (EXPERTS, D, FF), D ** -0.5, 0.09375, ((0, 4), (2, 8)))
    w_down = noise(arg_keys[12], (EXPERTS, FF, D), FF ** -0.5, 0.046875, ((0, 4), (1, 8)))
    return {"queries": queries, "keys": keys, "values": values, "block_of_slot": block_of_slot, "lengths": lengths, "out_proj": out_proj, "residual": residual, "norm_gain": norm_gain, "router": router, "routes": routes, "w_gate": w_gate, "w_up": w_up, "w_down": w_down}


masked_score = -1e+30

def reference(queries, keys, values, block_of_slot, lengths, out_proj, residual, norm_gain, router, routes, w_gate, w_up, w_down):
    per_kv = HEADS // KV_HEADS
    grouped = queries.astype(jnp.float32).reshape(REQUESTS, KV_HEADS, per_kv, HEAD_DIM)
    scores = jnp.einsum('rkgd,rlkd->rkgl', grouped, keys.astype(jnp.float32), precision=lax.Precision.HIGHEST) * HEAD_DIM ** (-0.5)
    offsets = jnp.arange(BLOCK, dtype=jnp.int32)
    position = (block_of_slot.astype(jnp.int32)[:, :, None] * BLOCK + offsets[None, None, :]).reshape(REQUESTS, CONTEXT)
    visible = (position < lengths.astype(jnp.int32)[:, None])[:, None, None, :]
    masked = jnp.where(visible, scores, masked_score)
    highest = lax.optimization_barrier(jnp.max(masked, axis=-1))
    probs = jnp.where(visible, jnp.exp(masked - highest[..., None]), 0.0)
    totals = lax.optimization_barrier(jnp.sum(probs, axis=-1))
    rounded = lax.optimization_barrier(probs.astype(jnp.bfloat16))
    weighted = jnp.einsum('rkgl,rlkd->rkgd', rounded.astype(jnp.float32), values.astype(jnp.float32), precision=lax.Precision.HIGHEST)
    attended = (weighted / totals[..., None]).astype(jnp.bfloat16).reshape(REQUESTS, HEADS * HEAD_DIM)
    hidden = residual.astype(jnp.float32) + jnp.dot(attended, out_proj, preferred_element_type=jnp.float32)
    meansq = lax.optimization_barrier(jnp.mean(hidden * hidden, axis=-1, keepdims=True))
    normed = (hidden * lax.rsqrt(meansq + 1e-05) * norm_gain.astype(jnp.float32)).astype(jnp.bfloat16)
    logits = jnp.dot(normed, router, preferred_element_type=jnp.float32)
    onehot = (routes.astype(jnp.int32)[:, :, None] == jnp.arange(EXPERTS, dtype=jnp.int32)[None, None, :]).astype(jnp.float32)
    chosen = lax.optimization_barrier(jnp.sum(onehot * logits[:, None, :], axis=-1))
    gate_probs = jax.nn.softmax(chosen, axis=-1)
    mixing = lax.optimization_barrier(jnp.sum(gate_probs[:, :, None] * onehot, axis=1))
    expert_mix = jnp.zeros((REQUESTS, D), jnp.float32)
    for expert in range(EXPERTS):
        gate_act = jnp.dot(normed, w_gate[expert], preferred_element_type=jnp.float32)
        upper = jnp.dot(normed, w_up[expert], preferred_element_type=jnp.float32)
        activated = (jax.nn.silu(gate_act) * upper).astype(jnp.bfloat16)
        expert_out = lax.optimization_barrier(jnp.dot(activated, w_down[expert], preferred_element_type=jnp.float32).astype(jnp.bfloat16))
        expert_mix = expert_mix + mixing[:, expert][:, None] * expert_out.astype(jnp.float32)
    return (hidden + expert_mix).astype(jnp.bfloat16)
```

```python
import functools

import jax
import jax.numpy as jnp
from jax import lax
from jax.experimental import pallas as pl
from jax.experimental.pallas import tpu as pltpu
from jax.sharding import PartitionSpec as P

BLOCK = 16
LANES = 128
EPS = 1e-05
masked_score = -1e30
ROUTE = ("outer", "seq", "expert")
f32 = jnp.float32
bf16 = jnp.bfloat16
MIB = 1 << 20
LIMIT = 7 * MIB
WORK = 4_000_000_000

VMEM = pl.BlockSpec(memory_space=pltpu.VMEM)
SMEM = pl.BlockSpec(memory_space=pltpu.SMEM)
HBM = pl.BlockSpec(memory_space=pl.ANY)


def exchange(value, axes, keys):
    count = 1
    for axis in axes:
        count *= lax.axis_size(axis)
    return [lax.ppermute(value, axes, [(i, i ^ key) for i in range(count)]) for key in keys]


def call(body, out_shape, in_specs, limit, scratch=(), cost=WORK, **more):
    many = isinstance(out_shape, (tuple, list))
    return pl.pallas_call(
        body,
        out_shape=out_shape,
        in_specs=in_specs,
        out_specs=[VMEM] * len(out_shape) if many else VMEM,
        scratch_shapes=list(scratch),
        compiler_params=pltpu.CompilerParams(vmem_limit_bytes=limit),
        cost_estimate=pl.CostEstimate(flops=cost, bytes_accessed=0, transcendentals=0),
        **more,
    )


def attend_local(*refs, kv_local, held):
    inputs, sources, refs = refs[:5], refs[5 : 5 + held], refs[5 + held :]
    out_ref, targets, refs = refs[0], refs[1 : 1 + held], refs[1 + held :]
    slot_ref, len_ref, q_ref, k_ref, v_ref, sems = refs
    pairs = [*zip(inputs, refs), *zip(sources, targets)]
    copies = [pltpu.make_async_copy(a, b, sems.at[i]) for i, (a, b) in enumerate(pairs)]
    for copy in copies:
        copy.start()
    rows, heads, dim = q_ref.shape
    entries = k_ref.shape[1]
    per_kv = heads // kv_local
    width = LANES // (2 * rows)
    lane = lax.broadcasted_iota(jnp.int32, (1, entries), 1)
    inside = lane // kv_local
    block_at = inside // BLOCK
    head = lax.broadcasted_iota(jnp.int32, (heads, entries), 0)
    own_kv = (head // per_kv) == (lane % kv_local)
    tag = lax.broadcasted_iota(jnp.int32, (heads, LANES), 1) // width
    stats = jnp.zeros((heads, LANES), f32)
    for copy in copies[:2]:
        copy.wait()
    seen = []
    for r in range(rows):
        start = jnp.zeros((1, entries), jnp.int32)
        for s in range(slot_ref.shape[1]):
            start = jnp.where(block_at == s, slot_ref[r, s] * BLOCK, start)
        seen.append(own_kv & ((start + inside % BLOCK) < len_ref[r]))
    for copy in copies[2:5]:
        copy.wait()
    for r in range(rows):
        scores = lax.dot_general(
            q_ref[r], k_ref[r], (((1,), (1,)), ((), ())), preferred_element_type=f32
        ) * (dim**-0.5)
        masked = jnp.where(seen[r], scores, masked_score)
        highest = jnp.max(masked, axis=1, keepdims=True)
        probs = jnp.where(seen[r], jnp.exp(masked - highest), 0.0)
        total = jnp.sum(probs, axis=1, keepdims=True)
        out_ref[pl.ds(r * heads, heads), :] = jnp.dot(
            probs.astype(bf16), v_ref[r], preferred_element_type=f32
        )
        stats = jnp.where(tag == 2 * r, highest, stats)
        stats = jnp.where(tag == 2 * r + 1, total, stats)
    out_ref[pl.ds(rows * heads, heads), :] = stats
    for copy in copies[5:]:
        copy.wait()


def project(*refs, rows, heads, parts):
    packs, (w_ref, res_ref, out_ref) = refs[:parts], refs[parts:]
    width = LANES // (2 * rows)
    dim = packs[0].shape[1]
    stats = [p[pl.ds(rows * heads, heads), :] for p in packs]
    lane_head = lax.broadcasted_iota(jnp.int32, (heads, heads * dim), 1) // dim
    row_head = lax.broadcasted_iota(jnp.int32, (heads, heads * dim), 0)
    flat = []
    for r in range(rows):
        highs = [s[:, 2 * r * width : 2 * r * width + 1] for s in stats]
        totals = [s[:, (2 * r + 1) * width : (2 * r + 1) * width + 1] for s in stats]
        top = functools.reduce(jnp.maximum, highs)
        scales = [jnp.exp(h - top) for h in highs]
        total = sum(t * c for t, c in zip(totals, scales))
        mixed = sum(p[pl.ds(r * heads, heads), :] * c for p, c in zip(packs, scales))
        spread = jnp.concatenate([mixed / total] * heads, axis=1)
        kept = jnp.where(lane_head == row_head, spread, 0.0)
        flat.append(jnp.sum(kept, axis=0, keepdims=True))
    attended = jnp.concatenate(flat, axis=0).astype(bf16)
    partial = jnp.dot(attended, w_ref[...], preferred_element_type=f32)
    first = (lax.axis_index("outer") + lax.axis_index("inner") == 0).astype(f32)
    out_ref[...] = (partial + res_ref[...].astype(f32) * first).astype(bf16)


def halves(width, start=0):
    core = lax.axis_index("inner")
    mine = pl.multiple_of(start + core * width, LANES)
    other = pl.multiple_of(start + (1 - core) * width, LANES)
    return pl.ds(mine, width), pl.ds(other, width)


def add_two(a_ref, b_ref, out_ref):
    out_ref[...] = (a_ref[...].astype(f32) + b_ref[...].astype(f32)).astype(out_ref.dtype)


def normalize(*refs, spans, pairs):
    parts = refs[: spans * pairs]
    gain_ref, router_ref, routes_ref, pack_ref, hid_ref, full_ref = refs[spans * pairs :]
    rows, cols = parts[0].shape
    model = spans * cols
    me = lax.axis_index("seq")
    for k in range(spans):
        held = sum(parts[k + spans * j][...].astype(f32) for j in range(pairs))
        if k == 0:
            hid_ref[...] = held
        full_ref[:, pl.ds(pl.multiple_of((me ^ k) * cols, cols), cols)] = held
    full = full_ref[...]
    meansq = jnp.sum(full * full, axis=1, keepdims=True) * (1.0 / model)
    scaled = full * lax.rsqrt(meansq + EPS)
    gain = gain_ref[...].astype(f32)
    normed = jnp.concatenate(
        [
            scaled[:, j * LANES : (j + 1) * LANES] * gain[j : j + 1, :]
            for j in range(model // LANES)
        ],
        axis=1,
    ).astype(bf16)
    logits = lax.dot_general(
        normed, router_ref[...], (((1,), (1,)), ((), ())), preferred_element_type=f32
    )
    expert = lax.broadcasted_iota(jnp.int32, logits.shape, 1)
    topk = routes_ref.shape[0]
    row = lax.broadcasted_iota(jnp.int32, logits.shape, 0)
    named = []
    for k in range(topk):
        route = jnp.zeros(logits.shape, jnp.int32)
        for r in range(rows):
            route = jnp.where(row == r, routes_ref[k, r], route)
        named.append(expert == route)
    chosen = [jnp.sum(jnp.where(n, logits, 0.0), axis=1, keepdims=True) for n in named]
    top = functools.reduce(jnp.maximum, chosen)
    raised = [jnp.exp(c - top) for c in chosen]
    total = sum(raised)
    mixing = sum(jnp.where(n, e / total, 0.0) for n, e in zip(named, raised))
    coarse = mixing.astype(bf16)
    fine = (mixing - coarse.astype(f32)).astype(bf16)
    pack_ref[:, pl.ds(0, model)] = normed
    pack_ref[:, pl.ds(model, 2 * LANES)] = jnp.zeros((rows, 2 * LANES), bf16)
    pack_ref[:, pl.ds(model, logits.shape[1])] = coarse
    pack_ref[:, pl.ds(model + LANES, logits.shape[1])] = fine


def experts(*refs, slots, experts_all, spans, step, depth, cuts):
    packs = refs[:slots]
    (gate_ref, up_ref, down_ref, keep_ref, send_ref, x_ref, mix_ref, y_ref, ring_ref, sems) = refs[
        slots:
    ]
    rows = packs[0].shape[0]
    local, model, units = up_ref.shape
    steps = units // step
    part = model // cuts
    pieces = local * steps * cuts
    me = lax.axis_index("expert")

    def place(t):
        return t // steps, pl.ds((t % steps) * step, step)

    def fetch(p):
        e, at = place(p // cuts)
        slot = p % depth
        start = (p % cuts) * part
        return pltpu.make_async_copy(
            down_ref.at[e, at, pl.ds(start, part)], ring_ref.at[slot], sems.at[slot]
        )

    for p in range(min(depth, pieces)):
        fetch(p).start()
    lane = lax.broadcasted_iota(jnp.int32, (rows, experts_all), 1)
    for k in range(slots):
        y_ref[pl.ds(k * rows, rows), :] = packs[k][:, pl.ds(0, model)].astype(f32)
        mixing = packs[k][:, pl.ds(model, experts_all)].astype(f32) + packs[k][
            :, pl.ds(model + LANES, experts_all)
        ].astype(f32)
        for e in range(local):
            mine = jnp.where(lane == me * local + e, mixing, 0.0)
            mix_ref[e, pl.ds(k * rows, rows), :] = jnp.broadcast_to(
                jnp.sum(mine, axis=1, keepdims=True), (rows, LANES)
            )
    x_ref[...] = y_ref[...].astype(bf16)
    y_ref[...] = jnp.zeros_like(y_ref)

    def raise_up(t):
        e, at = place(t)
        gate = jnp.dot(x_ref[...], gate_ref[e, :, at], preferred_element_type=f32)
        upper = jnp.dot(x_ref[...], up_ref[e, :, at], preferred_element_type=f32)
        weight = mix_ref[e][:, 0:1]
        return (gate * jax.nn.sigmoid(gate) * upper * weight).astype(bf16)

    def bring_down(t, active):
        for p in range(t * cuts, (t + 1) * cuts):
            at = pl.ds((p % cuts) * part, part)
            fetch(p).wait()
            y_ref[:, at] += jnp.dot(active, ring_ref[p % depth], preferred_element_type=f32)
            if p + depth < pieces:
                fetch(p + depth).start()

    last = local * steps
    active = raise_up(0)
    for t in range(1, last):
        fresh = raise_up(t)
        bring_down(t - 1, active)
        active = fresh
    bring_down(last - 1, active)
    half = model // spans // 2
    for i in range(spans):
        mine, other = halves(half, 2 * half * i)
        keep_ref[i] = y_ref[:, mine]
        send_ref[i] = y_ref[:, other].astype(bf16)


def scatter(keep_ref, got_ref, out_ref, *, outers, slots):
    spans = keep_ref.shape[0]
    rows = out_ref.shape[1]
    me = lax.axis_index("expert")
    for i in range(spans):
        held = keep_ref[i] + got_ref[i].astype(f32)
        for k in range(slots):
            piece = held[k * rows : (k + 1) * rows].astype(bf16)
            for j in range(outers):
                out_ref[(j * spans + i) * slots + (me ^ k)] = piece


def sum_first(in_ref, out_ref):
    out_ref[...] = jnp.sum(in_ref[...].astype(f32), axis=0).astype(out_ref.dtype)


def finish(hid_ref, mine_ref, other_ref, out_ref):
    for mix_ref, cols in zip((mine_ref, other_ref), halves(mine_ref.shape[1])):
        out_ref[:, cols] = (hid_ref[:, cols] + mix_ref[...].astype(f32)).astype(bf16)


def shards(
    queries,
    keys,
    values,
    block_of_slot,
    lengths,
    out_proj,
    residual,
    norm_gain,
    router,
    routes,
    w_gate,
    w_up,
    w_down,
):
    rows, heads, dim = queries.shape
    span_len, kv_local = keys.shape[1:3]
    outers, spans, slots = (lax.axis_size(a) for a in ROUTE)
    cols = out_proj.shape[1]
    model = spans * cols
    shape = jax.ShapeDtypeStruct
    kept = [out_proj, residual, norm_gain.reshape(model // LANES, LANES), router.T]
    hbm = functools.partial(pltpu.with_memory_space_constraint, memory_space=pltpu.HBM)
    flat = (rows, span_len * kv_local, dim)
    pack, out_proj, residual, gain, router_t = call(
        functools.partial(attend_local, kv_local=kv_local, held=len(kept)),
        [shape((rows * heads + heads, dim), f32)]
        + [pltpu.VMEM(a.shape, a.dtype) for a in kept],
        [HBM] * (5 + len(kept)),
        2 * MIB,
        [
            pltpu.SMEM(block_of_slot.shape, jnp.int32),
            pltpu.SMEM(lengths.shape, jnp.int32),
            pltpu.VMEM(queries.shape, bf16),
            pltpu.VMEM(flat, bf16),
            pltpu.VMEM(flat, bf16),
            pltpu.SemaphoreType.DMA((5 + len(kept),)),
        ],
        name="attend",
    )(
        hbm(block_of_slot),
        hbm(lengths),
        hbm(queries),
        hbm(keys.reshape(flat)),
        hbm(values.reshape(flat)),
        *[hbm(a) for a in kept],
    )
    packs = [pack] + exchange(pack, ("seq",), range(1, spans))
    partial = call(
        functools.partial(project, rows=rows, heads=heads, parts=spans),
        shape((rows, cols), bf16),
        [VMEM] * (spans + 2),
        1 * MIB,
        name="project",
    )(*packs, out_proj, residual)
    (other,) = exchange(partial, ("inner",), [1])
    paired = call(
        add_two, shape((rows, cols), bf16), [VMEM] * 2, 1 * MIB, name="pair"
    )(partial, other)
    keys_xy = [j * 2 * spans + k for j in range(outers) for k in range(spans)]
    pieces = [paired] + exchange(paired, ("outer", "inner", "seq"), keys_xy[1:])
    packet, hidden = call(
        functools.partial(normalize, spans=spans, pairs=outers),
        (shape((rows, model + 2 * LANES), bf16), shape((rows, cols), f32)),
        [VMEM] * (len(pieces) + 2) + [SMEM],
        1 * MIB,
        [pltpu.VMEM((rows, model), f32)],
        name="normalize",
    )(*pieces, gain, router_t, routes.T)
    packets = [packet] + exchange(packet, ("expert",), range(1, slots))
    local, _, units = w_up.shape
    step = 256 if units % 256 == 0 else units
    cuts, depth = 4, 9
    depth = min(depth, local * (units // step) * cuts)
    everyone = rows * slots
    keep, send = call(
        functools.partial(
            experts,
            slots=slots,
            experts_all=router.shape[1],
            spans=spans,
            step=step,
            depth=depth,
            cuts=cuts,
        ),
        (
            pltpu.VMEM((spans, everyone, cols // 2), f32),
            pltpu.VMEM((spans, everyone, cols // 2), bf16),
        ),
        [VMEM] * slots + [VMEM, VMEM, HBM],
        LIMIT,
        [
            pltpu.VMEM((everyone, model), bf16),
            pltpu.VMEM((local, everyone, LANES), f32),
            pltpu.VMEM((everyone, model), f32),
            pltpu.VMEM((depth, step, model // cuts), bf16),
            pltpu.SemaphoreType.DMA((depth,)),
        ],
        name="experts",
    )(
        *[pltpu.with_memory_space_constraint(p, pltpu.VMEM) for p in packets],
        pltpu.with_memory_space_constraint(w_gate, pltpu.VMEM),
        pltpu.with_memory_space_constraint(w_up, pltpu.VMEM),
        pltpu.with_memory_space_constraint(w_down, pltpu.HBM),
    )
    (back,) = exchange(send, ("inner",), [1])
    packet = call(
        functools.partial(scatter, outers=outers, slots=slots),
        shape((outers * spans * slots, rows, cols // 2), bf16),
        [VMEM] * 2,
        1 * MIB,
        name="scatter",
    )(keep, back)
    arrived = lax.all_to_all(packet, ROUTE, 0, 0, tiled=True)
    mine = call(sum_first, shape((rows, cols // 2), bf16), [VMEM], 1 * MIB, name="total")(arrived)
    (other,) = exchange(mine, ("inner",), [1])
    return call(finish, shape((rows, cols), bf16), [VMEM] * 3, 1 * MIB, name="finish")(
        hidden, mine, other
    )


def solution(mesh):
    groups, spans, slots = (mesh.shape[a] for a in ("group", "seq", "expert"))
    group = ("outer", "inner")
    split = jax.sharding.Mesh(
        mesh.devices.reshape(groups // 2, 2, spans, slots), (*group, "seq", "expert")
    )
    return jax.shard_map(
        shards,
        mesh=split,
        in_specs=(
            P("expert", group, None),
            P("expert", "seq", group, None),
            P("expert", "seq", group, None),
            P("expert", "seq"),
            P("expert"),
            P(group, "seq"),
            P("expert", "seq"),
            P(),
            P(),
            P("expert", None),
            P("expert", None, (*group, "seq")),
            P("expert", None, (*group, "seq")),
            P("expert", (*group, "seq"), None),
        ),
        out_specs=P("expert", "seq"),
        check_vma=False,
    )
```

```python
import functools

import jax
import jax.numpy as jnp
from jax import lax
from jax.experimental import pallas as pl
from jax.experimental.pallas import tpu as pltpu
from jax.sharding import PartitionSpec as P

BLOCK = 16
LANES = 128
EPS = 1e-05
masked_score = -1e30
ROUTE = ("outer", "seq", "expert")
f32 = jnp.float32
bf16 = jnp.bfloat16
MIB = 1 << 20
LIMIT = 7 * MIB
WORK = 4_000_000_000

VMEM = pl.BlockSpec(memory_space=pltpu.VMEM)
SMEM = pl.BlockSpec(memory_space=pltpu.SMEM)
HBM = pl.BlockSpec(memory_space=pl.ANY)


def exchange(value, axes, keys):
    count = 1
    for axis in axes:
        count *= lax.axis_size(axis)
    return [lax.ppermute(value, axes, [(i, i ^ key) for i in range(count)]) for key in keys]


def split_exchange(value, axis, core):
    count = lax.axis_size(axis)
    held = []
    for low in range(2, count, 2):
        pairs = [
            (c * count + i, c * count + (i ^ (low + 1 - c))) for c in range(2) for i in range(count)
        ]
        fetched = lax.ppermute(value, (core, axis), pairs)
        held.append((fetched, exchange(fetched, (core,), [1])[0]))
    (near,) = exchange(value, (axis,), [1])
    return [near] + [part for pair in held for part in pair]


def split_plane(value, outers, spans):
    axes = ("outer", "inner", "seq")
    if (outers, spans) != (2, 2):
        keys = [j * 2 * spans + k for j in range(outers) for k in range(spans)]
        return exchange(value, axes, keys[1:])
    count = 2 * outers * spans
    far = 2 * spans + 1
    pairs = [(i, i ^ (1 if i // spans % 2 else far)) for i in range(count)]
    fetched = lax.ppermute(value, axes, pairs)
    (beside,) = exchange(value, axes, [2 * spans])
    (swapped,) = exchange(fetched, ("inner",), [1])
    return [fetched, beside, swapped]


def call(body, out_shape, in_specs, limit, scratch=(), cost=WORK, **more):
    many = isinstance(out_shape, (tuple, list))
    return pl.pallas_call(
        body,
        out_shape=out_shape,
        in_specs=in_specs,
        out_specs=[VMEM] * len(out_shape) if many else VMEM,
        scratch_shapes=list(scratch),
        compiler_params=pltpu.CompilerParams(vmem_limit_bytes=limit),
        cost_estimate=pl.CostEstimate(flops=cost, bytes_accessed=0, transcendentals=0),
        **more,
    )


def attend_local(*refs, kv_local, held):
    inputs, sources, refs = refs[:5], refs[5 : 5 + held], refs[5 + held :]
    out_ref, targets, refs = refs[0], refs[1 : 1 + held], refs[1 + held :]
    slot_ref, len_ref, q_ref, k_ref, v_ref, sems = refs
    pairs = [*zip(inputs, refs), *zip(sources, targets)]
    copies = [pltpu.make_async_copy(a, b, sems.at[i]) for i, (a, b) in enumerate(pairs)]
    for copy in copies:
        copy.start()
    rows, heads, dim = q_ref.shape
    entries = k_ref.shape[1]
    per_kv = heads // kv_local
    width = LANES // (2 * rows)
    lane = lax.broadcasted_iota(jnp.int32, (1, entries), 1)
    inside = lane // kv_local
    block_at = inside // BLOCK
    head = lax.broadcasted_iota(jnp.int32, (heads, entries), 0)
    own_kv = (head // per_kv) == (lane % kv_local)
    tag = lax.broadcasted_iota(jnp.int32, (heads, LANES), 1) // width
    stats = jnp.zeros((heads, LANES), f32)
    for copy in copies[:2]:
        copy.wait()
    seen = []
    for r in range(rows):
        start = jnp.zeros((1, entries), jnp.int32)
        for s in range(slot_ref.shape[1]):
            start = jnp.where(block_at == s, slot_ref[r, s] * BLOCK, start)
        seen.append(own_kv & ((start + inside % BLOCK) < len_ref[r]))
    for copy in copies[2:5]:
        copy.wait()
    for r in range(rows):
        scores = lax.dot_general(
            q_ref[r], k_ref[r], (((1,), (1,)), ((), ())), preferred_element_type=f32
        ) * (dim**-0.5)
        masked = jnp.where(seen[r], scores, masked_score)
        highest = jnp.max(masked, axis=1, keepdims=True)
        probs = jnp.where(seen[r], jnp.exp(masked - highest), 0.0)
        total = jnp.sum(probs, axis=1, keepdims=True)
        out_ref[pl.ds(r * heads, heads), :] = jnp.dot(
            probs.astype(bf16), v_ref[r], preferred_element_type=f32
        )
        stats = jnp.where(tag == 2 * r, highest, stats)
        stats = jnp.where(tag == 2 * r + 1, total, stats)
    out_ref[pl.ds(rows * heads, heads), :] = stats
    for copy in copies[5:]:
        copy.wait()


def project(*refs, rows, heads, parts):
    packs, (w_ref, res_ref, out_ref) = refs[:parts], refs[parts:]
    width = LANES // (2 * rows)
    dim = packs[0].shape[1]
    stats = [p[pl.ds(rows * heads, heads), :] for p in packs]
    lane_head = lax.broadcasted_iota(jnp.int32, (heads, heads * dim), 1) // dim
    row_head = lax.broadcasted_iota(jnp.int32, (heads, heads * dim), 0)
    flat = []
    for r in range(rows):
        highs = [s[:, 2 * r * width : 2 * r * width + 1] for s in stats]
        totals = [s[:, (2 * r + 1) * width : (2 * r + 1) * width + 1] for s in stats]
        top = functools.reduce(jnp.maximum, highs)
        scales = [jnp.exp(h - top) for h in highs]
        total = sum(t * c for t, c in zip(totals, scales))
        mixed = sum(p[pl.ds(r * heads, heads), :] * c for p, c in zip(packs, scales))
        spread = jnp.concatenate([mixed / total] * heads, axis=1)
        kept = jnp.where(lane_head == row_head, spread, 0.0)
        flat.append(jnp.sum(kept, axis=0, keepdims=True))
    attended = jnp.concatenate(flat, axis=0).astype(bf16)
    partial = jnp.dot(attended, w_ref[...], preferred_element_type=f32)
    first = (lax.axis_index("outer") + lax.axis_index("inner") == 0).astype(f32)
    out_ref[...] = (partial + res_ref[...].astype(f32) * first).astype(bf16)


def halves(width, start=0):
    core = lax.axis_index("inner")
    mine = pl.multiple_of(start + core * width, LANES)
    other = pl.multiple_of(start + (1 - core) * width, LANES)
    return pl.ds(mine, width), pl.ds(other, width)


def add_two(a_ref, b_ref, out_ref):
    out_ref[...] = (a_ref[...].astype(f32) + b_ref[...].astype(f32)).astype(out_ref.dtype)


def normalize(*refs, spans, pairs):
    parts = refs[: spans * pairs]
    gain_ref, router_ref, routes_ref, pack_ref, hid_ref, full_ref = refs[spans * pairs :]
    rows, cols = parts[0].shape
    model = spans * cols
    me = lax.axis_index("seq")
    for k in range(spans):
        held = sum(parts[k + spans * j][...].astype(f32) for j in range(pairs))
        if k == 0:
            hid_ref[...] = held
        full_ref[:, pl.ds(pl.multiple_of((me ^ k) * cols, cols), cols)] = held
    full = full_ref[...]
    meansq = jnp.sum(full * full, axis=1, keepdims=True) * (1.0 / model)
    scaled = full * lax.rsqrt(meansq + EPS)
    gain = gain_ref[...].astype(f32)
    normed = jnp.concatenate(
        [
            scaled[:, j * LANES : (j + 1) * LANES] * gain[j : j + 1, :]
            for j in range(model // LANES)
        ],
        axis=1,
    ).astype(bf16)
    logits = lax.dot_general(
        normed, router_ref[...], (((1,), (1,)), ((), ())), preferred_element_type=f32
    )
    expert = lax.broadcasted_iota(jnp.int32, logits.shape, 1)
    topk = routes_ref.shape[0]
    row = lax.broadcasted_iota(jnp.int32, logits.shape, 0)
    named = []
    for k in range(topk):
        route = jnp.zeros(logits.shape, jnp.int32)
        for r in range(rows):
            route = jnp.where(row == r, routes_ref[k, r], route)
        named.append(expert == route)
    chosen = [jnp.sum(jnp.where(n, logits, 0.0), axis=1, keepdims=True) for n in named]
    top = functools.reduce(jnp.maximum, chosen)
    raised = [jnp.exp(c - top) for c in chosen]
    total = sum(raised)
    mixing = sum(jnp.where(n, e / total, 0.0) for n, e in zip(named, raised))
    coarse = mixing.astype(bf16)
    fine = (mixing - coarse.astype(f32)).astype(bf16)
    pack_ref[:, pl.ds(0, model)] = normed
    pack_ref[:, pl.ds(model, 2 * LANES)] = jnp.zeros((rows, 2 * LANES), bf16)
    pack_ref[:, pl.ds(model, logits.shape[1])] = coarse
    pack_ref[:, pl.ds(model + LANES, logits.shape[1])] = fine


def experts(*refs, slots, spans, step, depth, cuts):
    packs = refs[:slots]
    (gate_ref, up_ref, down_ref, keep_ref, send_ref, x_ref, mix_ref, y_ref, ring_ref, sems) = refs[
        slots:
    ]
    rows = packs[0].shape[0]
    local, model, units = up_ref.shape
    steps = units // step
    part = model // cuts
    pieces = local * steps * cuts
    me = lax.axis_index("expert")

    def place(t):
        return t // steps, pl.ds((t % steps) * step, step)

    def fetch(p):
        e, at = place(p // cuts)
        slot = p % depth
        start = (p % cuts) * part
        return pltpu.make_async_copy(
            down_ref.at[e, at, pl.ds(start, part)], ring_ref.at[slot], sems.at[slot]
        )

    for p in range(min(depth, pieces)):
        fetch(p).start()
    lane = lax.broadcasted_iota(jnp.int32, (rows, LANES), 1)
    south = lax.axis_index("inner") == 0
    for k in range(slots):
        pack = packs[k][...].astype(f32)
        if k >= 2:
            pack = jnp.where(south, packs[k ^ 1][...].astype(f32), pack)
        y_ref[pl.ds(k * rows, rows), :] = pack[:, :model]
        mixing = pack[:, model : model + LANES] + pack[:, model + LANES :]
        for e in range(local):
            mine = jnp.where(lane == me * local + e, mixing, 0.0)
            mix_ref[e, pl.ds(k * rows, rows), :] = jnp.broadcast_to(
                jnp.sum(mine, axis=1, keepdims=True), (rows, LANES)
            )
    x_ref[...] = y_ref[...].astype(bf16)
    y_ref[...] = jnp.zeros_like(y_ref)

    def raise_up(t):
        e, at = place(t)
        gate = jnp.dot(x_ref[...], gate_ref[e, :, at], preferred_element_type=f32)
        upper = jnp.dot(x_ref[...], up_ref[e, :, at], preferred_element_type=f32)
        weight = mix_ref[e][:, 0:1]
        return (gate * jax.nn.sigmoid(gate) * upper * weight).astype(bf16)

    def bring_down(t, active):
        for p in range(t * cuts, (t + 1) * cuts):
            at = pl.ds((p % cuts) * part, part)
            fetch(p).wait()
            y_ref[:, at] += jnp.dot(active, ring_ref[p % depth], preferred_element_type=f32)
            if p + depth < pieces:
                fetch(p + depth).start()

    last = local * steps
    active = raise_up(0)
    for t in range(1, last):
        fresh = raise_up(t)
        bring_down(t - 1, active)
        active = fresh
    bring_down(last - 1, active)
    half = model // spans // 2
    for i in range(spans):
        mine, other = halves(half, 2 * half * i)
        keep_ref[i] = y_ref[:, mine]
        send_ref[i] = y_ref[:, other].astype(bf16)


def scatter(keep_ref, got_ref, out_ref, *, outers, slots):
    spans = keep_ref.shape[0]
    rows = out_ref.shape[1]
    me = lax.axis_index("expert")
    for i in range(spans):
        held = keep_ref[i] + got_ref[i].astype(f32)
        for k in range(slots):
            piece = held[k * rows : (k + 1) * rows].astype(bf16)
            for j in range(outers):
                out_ref[(j * spans + i) * slots + (me ^ k)] = piece


def sum_first(in_ref, out_ref):
    out_ref[...] = jnp.sum(in_ref[...].astype(f32), axis=0).astype(out_ref.dtype)


def finish(hid_ref, mine_ref, other_ref, out_ref):
    for mix_ref, cols in zip((mine_ref, other_ref), halves(mine_ref.shape[1])):
        out_ref[:, cols] = (hid_ref[:, cols] + mix_ref[...].astype(f32)).astype(bf16)


def shards(
    queries,
    keys,
    values,
    block_of_slot,
    lengths,
    out_proj,
    residual,
    norm_gain,
    router,
    routes,
    w_gate,
    w_up,
    w_down,
):
    rows, heads, dim = queries.shape
    span_len, kv_local = keys.shape[1:3]
    outers, spans, slots = (lax.axis_size(a) for a in ROUTE)
    cols = out_proj.shape[1]
    model = spans * cols
    shape = jax.ShapeDtypeStruct
    kept = [out_proj, residual, norm_gain.reshape(model // LANES, LANES), router.T]
    hbm = functools.partial(pltpu.with_memory_space_constraint, memory_space=pltpu.HBM)
    flat = (rows, span_len * kv_local, dim)
    pack, out_proj, residual, gain, router_t = call(
        functools.partial(attend_local, kv_local=kv_local, held=len(kept)),
        [shape((rows * heads + heads, dim), f32)]
        + [pltpu.VMEM(a.shape, a.dtype) for a in kept],
        [HBM] * (5 + len(kept)),
        2 * MIB,
        [
            pltpu.SMEM(block_of_slot.shape, jnp.int32),
            pltpu.SMEM(lengths.shape, jnp.int32),
            pltpu.VMEM(queries.shape, bf16),
            pltpu.VMEM(flat, bf16),
            pltpu.VMEM(flat, bf16),
            pltpu.SemaphoreType.DMA((5 + len(kept),)),
        ],
        name="attend",
    )(
        hbm(block_of_slot),
        hbm(lengths),
        hbm(queries),
        hbm(keys.reshape(flat)),
        hbm(values.reshape(flat)),
        *[hbm(a) for a in kept],
    )
    packs = [pack] + exchange(pack, ("seq",), range(1, spans))
    partial = call(
        functools.partial(project, rows=rows, heads=heads, parts=spans),
        shape((rows, cols), bf16),
        [VMEM] * (spans + 2),
        1 * MIB,
        name="project",
    )(*packs, out_proj, residual)
    (other,) = exchange(partial, ("inner",), [1])
    paired = call(
        add_two, shape((rows, cols), bf16), [VMEM] * 2, 1 * MIB, name="pair"
    )(partial, other)
    pieces = [paired] + split_plane(paired, outers, spans)
    packet, hidden = call(
        functools.partial(normalize, spans=spans, pairs=outers),
        (shape((rows, model + 2 * LANES), bf16), shape((rows, cols), f32)),
        [VMEM] * (len(pieces) + 2) + [SMEM],
        1 * MIB,
        [pltpu.VMEM((rows, model), f32)],
        name="normalize",
    )(*pieces, gain, router_t, routes.T)
    packets = [packet] + split_exchange(packet, "expert", "inner")
    local, _, units = w_up.shape
    step = 256 if units % 256 == 0 else units
    cuts, depth = 2, 5
    depth = min(depth, local * (units // step) * cuts)
    everyone = rows * slots
    keep, send = call(
        functools.partial(
            experts,
            slots=slots,
            spans=spans,
            step=step,
            depth=depth,
            cuts=cuts,
        ),
        (
            pltpu.VMEM((spans, everyone, cols // 2), f32),
            pltpu.VMEM((spans, everyone, cols // 2), bf16),
        ),
        [VMEM] * slots + [VMEM, VMEM, HBM],
        LIMIT,
        [
            pltpu.VMEM((everyone, model), bf16),
            pltpu.VMEM((local, everyone, LANES), f32),
            pltpu.VMEM((everyone, model), f32),
            pltpu.VMEM((depth, step, model // cuts), bf16),
            pltpu.SemaphoreType.DMA((depth,)),
        ],
        name="experts",
    )(
        *[pltpu.with_memory_space_constraint(p, pltpu.VMEM) for p in packets],
        pltpu.with_memory_space_constraint(w_gate, pltpu.VMEM),
        pltpu.with_memory_space_constraint(w_up, pltpu.VMEM),
        pltpu.with_memory_space_constraint(w_down, pltpu.HBM),
    )
    (back,) = exchange(send, ("inner",), [1])
    packet = call(
        functools.partial(scatter, outers=outers, slots=slots),
        shape((outers * spans * slots, rows, cols // 2), bf16),
        [VMEM] * 2,
        1 * MIB,
        name="scatter",
    )(keep, back)
    arrived = lax.all_to_all(packet, ROUTE, 0, 0, tiled=True)
    mine = call(sum_first, shape((rows, cols // 2), bf16), [VMEM], 1 * MIB, name="total")(arrived)
    (other,) = exchange(mine, ("inner",), [1])
    return call(finish, shape((rows, cols), bf16), [VMEM] * 3, 1 * MIB, name="finish")(
        hidden, mine, other
    )


def solution(mesh):
    groups, spans, slots = (mesh.shape[a] for a in ("group", "seq", "expert"))
    group = ("outer", "inner")
    split = jax.sharding.Mesh(
        mesh.devices.reshape(groups // 2, 2, spans, slots), (*group, "seq", "expert")
    )
    return jax.shard_map(
        shards,
        mesh=split,
        in_specs=(
            P("expert", group, None),
            P("expert", "seq", group, None),
            P("expert", "seq", group, None),
            P("expert", "seq"),
            P("expert"),
            P(group, "seq"),
            P("expert", "seq"),
            P(),
            P(),
            P("expert", None),
            P("expert", None, (*group, "seq")),
            P("expert", None, (*group, "seq")),
            P("expert", (*group, "seq"), None),
        ),
        out_specs=P("expert", "seq"),
        check_vma=False,
    )
```
